512 devices in a mesh: row: 32 (over z_hi, x, y), col: 16 (over z_lo, core).
Axes of the slice: x: 4, y: 4, z: 16 (z_hi: 2, z_lo: 8; z = z_hi * 8 + z_lo), core: 2. Of those that a mesh axis runs over, the one named last changes fastest.
Arguments:
- replicas: bfloat16 [10240, 40960], P('row', 'col'), may hold values from -24 to 24
- factor_seeds: int32 [8, 8, 2, 2], replicated, may hold values from 0 to 8190
- edge_counts: int32 [8, 8, 2], replicated, may hold values from 1 to 4
Outputs:
- update: float32 [10240, 40960], P('row', 'col')
The draws below stay inside these ranges and needn't reach their ends.
All inputs are finite; a program needn't handle non-finite values.
Results may differ from the reference program's by a relative error of at most 0.0003.
Values sent between devices are 32-bit elements; how exact they have to be, the bound alone decides.
A program may use at most 64 MiB of HBM per device.

```python
import jax
import jax.numpy as jnp
from jax import lax

D_MODEL = 1280
HIDDEN_SIZE = 5120
RANK = 2
ROUNDS = 2
GRAPH_ROWS = 8
GRAPH_COLS = 8


def touch_ends(entries, own_key, low, high):
    extent = entries.shape
    place = [jax.random.randint(jax.random.fold_in(own_key, axis), (), 0, extent[axis]) for axis in range(len(extent))]
    entries = entries.at[tuple(place)].set(low)
    longest = extent.index(max(extent))
    place[longest] = (place[longest] + 1) % extent[longest]
    return entries.at[tuple(place)].set(high)


def steps_of(rng, shape, shards, low, top_value):
    loudness = 1.0
    for dim, shards_of in shards:
        draws = jax.random.uniform(jax.random.fold_in(jax.random.fold_in(rng, 6), dim), (shards_of,), jnp.float32, low / len(shards), top_value / len(shards))
        loudness = loudness * jnp.repeat(jnp.exp(draws), shape[dim] // shards_of).reshape((-1,) + (1,) * (len(shape) - 1 - dim))
    return loudness


def centred(key, dims, width, limit, pieces=(), kind=jnp.bfloat16):
    entries = width * jax.random.normal(key, dims, jnp.float32)
    if pieces:
        entries = entries * steps_of(key, dims, pieces, -0.22, 0.18)
    return jnp.clip(entries, -limit, limit).astype(kind)


def setup_inputs(seed: int = 0) -> dict:
    key_of = jax.random.split(jax.random.key(seed), 4)
    return {
        "replicas": centred(key_of[0], (GRAPH_ROWS * D_MODEL, GRAPH_COLS * HIDDEN_SIZE), 4.0, 24.0, ((0, 32), (1, 16))),
        "factor_seeds": touch_ends(jax.random.randint(key_of[1], (GRAPH_ROWS, GRAPH_COLS, 2, RANK), 0, 8191), jax.random.fold_in(key_of[1], 1), 0, 8190).astype(jnp.int32),
        "edge_counts": touch_ends(jax.random.randint(key_of[2], (GRAPH_ROWS, GRAPH_COLS, 2), 1, 5), jax.random.fold_in(key_of[2], 1), 1, 4).astype(jnp.int32),
    }


highest = lax.Precision.HIGHEST
epsilon = 1e-06

def start_factors(factor_seeds):
    column = jnp.arange(HIDDEN_SIZE, dtype=jnp.int32)
    square = column * column % 8191
    residue = (square * (factor_seeds[..., None] + 1) + column * 17) % 8191
    return residue.astype(jnp.float32) * (2.0 / 8191.0) - 1.0

def images_of(replica_blocks, update_blocks, vectors):
    if update_blocks is None:

        def one_row(row_items):
            row_block, row_vectors = row_items
            return jnp.einsum('cjm,kcm->cjk', row_vectors, row_block.astype(jnp.float32), precision=highest)
        return lax.map(one_row, (replica_blocks, vectors))

    def one_row_more(row_items):
        row_block, row_update, row_vectors = row_items
        leading = jnp.einsum('cjm,kcm->cjk', row_vectors, row_block.astype(jnp.float32), precision=highest)
        return leading + jnp.einsum('cjm,kcm->cjk', row_vectors, row_update, precision=highest)
    return lax.map(one_row_more, (replica_blocks, update_blocks, vectors))

def projections_of(replica_blocks, update_blocks, directions):
    if update_blocks is None:

        def one_row(row_items):
            row_block, row_vectors = row_items
            return jnp.einsum('cjk,kcm->cjm', row_vectors, row_block.astype(jnp.float32), precision=highest)
        return lax.map(one_row, (replica_blocks, directions))

    def one_row_more(row_items):
        row_block, row_update, row_vectors = row_items
        leading = jnp.einsum('cjk,kcm->cjm', row_vectors, row_block.astype(jnp.float32), precision=highest)
        return leading + jnp.einsum('cjk,kcm->cjm', row_vectors, row_update, precision=highest)
    return lax.map(one_row_more, (replica_blocks, update_blocks, directions))

def orthonormal(values):
    leading = values[..., 0, :]
    second = values[..., 1, :]
    lead_norm = lax.optimization_barrier(jnp.sum(leading * leading, -1, keepdims=True))
    leading = leading / jnp.sqrt(lead_norm + epsilon)
    correlation = lax.optimization_barrier(jnp.sum(leading * second, -1, keepdims=True))
    second = second - correlation * leading
    rest_norm = lax.optimization_barrier(jnp.sum(second * second, -1, keepdims=True))
    second = second / jnp.sqrt(rest_norm + epsilon)
    return jnp.stack([leading, second], -2)

def reference(replicas, factor_seeds, edge_counts):
    replica_blocks = replicas.reshape(GRAPH_ROWS, D_MODEL, GRAPH_COLS, HIDDEN_SIZE)
    initial = start_factors(factor_seeds)
    factors = [initial[:, :, 0], initial[:, :, 1]]
    scales = [edge_counts[:, :, 0].astype(jnp.float32) / 16.0, edge_counts[:, :, 1].astype(jnp.float32) / 16.0]
    update_blocks = None
    for round_index in range(ROUNDS):
        left_factors = []
        right_factors = []
        fresh_list = []
        for graph_axis in range(2):
            vectors = factors[graph_axis]
            own_images = images_of(replica_blocks, update_blocks, vectors)
            other_images = jnp.roll(images_of(replica_blocks, update_blocks, jnp.roll(vectors, 1, graph_axis)), -1, graph_axis)
            directions = orthonormal(own_images - other_images)
            mine = projections_of(replica_blocks, update_blocks, directions)
            theirs = jnp.roll(projections_of(replica_blocks, update_blocks, jnp.roll(directions, 1, graph_axis)), -1, graph_axis)
            fresh_factors = mine - theirs
            fresh_list.append(fresh_factors)
            edge_scale = scales[graph_axis][:, :, None, None]
            left_factors += [directions, jnp.roll(directions, 1, graph_axis)]
            right_factors += [-edge_scale * fresh_factors, jnp.roll(edge_scale * fresh_factors, 1, graph_axis)]
        factors = fresh_list
        left_stack = jnp.stack(left_factors, 2)
        right_stack = jnp.stack(right_factors, 2)

        def one_row(row_items):
            return jnp.einsum('cejk,cejm->kcm', row_items[0], row_items[1], precision=highest)
        correction = lax.map(one_row, (left_stack, right_stack))
        update_blocks = correction if update_blocks is None else update_blocks + correction
    return update_blocks.reshape(GRAPH_ROWS * D_MODEL, GRAPH_COLS * HIDDEN_SIZE)
```

```python
import functools

import jax
import jax.numpy as jnp
from jax import lax
from jax.experimental import pallas as pl
from jax.experimental.pallas import tpu as pltpu
from jax.sharding import PartitionSpec as P

ROUNDS = 2
ROW_SHARDS = 4
COL_SHARDS = 2
SLOTS = 4
RANK = 2
EDGE_ROWS = SLOTS * RANK
PRIME = 8191
EPSILON = 1e-06
MESH_ID = pl.DeviceIdType.MESH
NT = (((1,), (1,)), ((), ()))
NN = (((1,), (0,)), ((), ()))
TN = (((0,), (0,)), ((), ()))


def product(left, right, dims):
    return lax.dot_general(left, right, dims, preferred_element_type=jnp.float32)


def halves(values):
    high = values.astype(jnp.bfloat16)
    return high, (values - high.astype(jnp.float32)).astype(jnp.bfloat16)


def stacked_halves(values):
    return jnp.concatenate(halves(values), axis=0)


def folded(values):
    return (values & PRIME) + (values >> 13)


def start_factors(seed_column, first_column, width):
    column = first_column + lax.broadcasted_iota(jnp.int32, (EDGE_ROWS, width), 1)
    square = folded(column * column)
    residue = folded(folded(square * (seed_column + 1) + column * 17))
    residue = jnp.where(residue >= PRIME, residue - PRIME, residue)
    return residue.astype(jnp.float32) * (2.0 / 8191.0) - 1.0


def column_of(scalars):
    row = lax.broadcasted_iota(jnp.int32, (EDGE_ROWS, 1), 0)
    values = jnp.full((EDGE_ROWS, 1), scalars[0])
    for index in range(1, EDGE_ROWS):
        values = jnp.where(row == index, scalars[index], values)
    return values


def partner_rows(values):
    row = lax.broadcasted_iota(jnp.int32, values.shape, 0)
    down = pltpu.roll(values, 1, 0)
    up = pltpu.roll(values, EDGE_ROWS - 1, 0)
    return jnp.where(row % 2 == 0, up, down)


def gram(directions):
    norm = jnp.sum(directions * directions, axis=1, keepdims=True)
    cross = jnp.sum(directions * partner_rows(directions), axis=1, keepdims=True)
    lane = lax.broadcasted_iota(jnp.int32, (EDGE_ROWS, 128), 1)
    return jnp.where(lane == 0, norm, jnp.where(lane == 1, cross, 0.0))


def normalizers(statistics):
    row = lax.broadcasted_iota(jnp.int32, (EDGE_ROWS, 128), 0)
    norm = jnp.broadcast_to(statistics[:, 0:1], (EDGE_ROWS, 128))
    cross = jnp.broadcast_to(statistics[:, 1:2], (EDGE_ROWS, 128))
    other = partner_rows(norm)
    first = row % 2 == 0
    lead = jnp.where(first, norm, other)
    rest = jnp.where(first, other, norm)
    share = jnp.where(cross == lead + EPSILON, 1.0, cross / (lead + EPSILON))
    left_over = (rest - share * cross) - share * (cross - share * lead)
    left_over = jnp.maximum(left_over, 0.0)
    scale = 1.0 / jnp.sqrt(jnp.where(first, lead, left_over) + EPSILON)
    share = jnp.where(first, 0.0, share)
    return scale[:, 0:1], share[:, 0:1]


def normalized(values, scale, share):
    return (values - share * partner_rows(values)) * scale


def rows_of(slabs):
    return jnp.concatenate([slabs[slot] for slot in range(SLOTS)], axis=0)


def consensus(
    x_hbm, seeds, counts, left_out, right_out, x, images, image_pair, image_near,
    stats, parts, parts_in, sums, sums_in, shares, x_sem, image_send, image_recv,
    stat_send, stat_recv, part_send, part_recv, sum_send, sum_recv, share_send, share_recv,
):
    local_rows, width = x.shape
    quarter = width // ROW_SHARDS
    graph_rows, graph_cols = seeds.shape[0], seeds.shape[1]
    row, col = lax.axis_index("row"), lax.axis_index("col")
    node_row, shard = row // ROW_SHARDS, row % ROW_SHARDS
    node_col, core = col // COL_SHARDS, col % COL_SHARDS
    below = (node_row + 1) % graph_rows
    above = (node_row + graph_rows - 1) % graph_rows
    right = (node_col + 1) % graph_cols
    left = (node_col + graph_cols - 1) % graph_cols
    neighbours = [(below, node_col), (above, node_col), (node_row, right), (node_row, left)]

    def device(node, at_shard, at_core):
        return (node[0] * ROW_SHARDS + at_shard, node[1] * COL_SHARDS + at_core)

    sibling = device((node_row, node_col), shard, 1 - core)
    shard_peers = [
        device((node_row, node_col), (shard + apart) % ROW_SHARDS, core)
        for apart in range(1, ROW_SHARDS)
    ]

    load = pltpu.make_async_copy(x_hbm, x, x_sem)
    load.start()
    barrier = pltpu.get_barrier_semaphore()
    partners = [device(node, shard, at) for node in neighbours for at in range(COL_SHARDS)]
    partners += [sibling] + shard_peers
    for partner in partners:
        pl.semaphore_signal(barrier, inc=1, device_id=partner, device_id_type=MESH_ID)

    owners = [(node_row, node_col, 0), (above, node_col, 0), (node_row, node_col, 1), (node_row, left, 1)]
    seed_column = column_of([seeds[r, c, a, k] for r, c, a in owners for k in range(RANK)])
    weight = column_of([counts[r, c, a] for r, c, a in owners for _ in range(RANK)])
    weight = weight.astype(jnp.float32) * (-1.0 / 16.0)
    factors = start_factors(seed_column, core * width, width)

    sent = []

    def send(source, target, send_sem, recv_sem, to):
        copy = pltpu.make_async_remote_copy(
            src_ref=source, dst_ref=target, send_sem=send_sem, recv_sem=recv_sem,
            device_id=to, device_id_type=MESH_ID,
        )
        copy.start()
        sent.append(copy)
        return copy

    lefts, rights = [], []
    load.wait()
    for turn in range(ROUNDS):
        factor_halves = stacked_halves(factors)
        image = product(factor_halves, x[...], NT)
        image = image[:EDGE_ROWS] + image[EDGE_ROWS:]
        if turn > 0:
            overlap = product(factor_halves, factor_halves, NT)
            overlap = overlap[:EDGE_ROWS] + overlap[EDGE_ROWS:]
            overlap = overlap[:, :EDGE_ROWS] + overlap[:, EDGE_ROWS:]
            weighted = weight * lefts[0]
            for g in range(EDGE_ROWS):
                image = image + overlap[:, g : g + 1] * weighted[g : g + 1, :]
        for slot in range(SLOTS):
            images[turn, slot] = image[RANK * slot : RANK * (slot + 1), :]
        if turn == 0:
            pl.semaphore_wait(barrier, len(partners))
        arrivals = []
        for slot, node in enumerate(neighbours):
            for at in range(COL_SHARDS):
                arrivals.append(
                    send(
                        images.at[turn, slot], image_near.at[turn, slot ^ 1, core],
                        image_send.at[turn, slot, at], image_recv.at[turn, slot ^ 1, core],
                        device(node, shard, at),
                    )
                )
        pair = send(images.at[turn], image_pair.at[turn], image_send.at[turn, SLOTS, 0], image_recv.at[turn, SLOTS, 0], sibling)
        pair.wait_recv()
        own = image + rows_of([image_pair[turn, slot] for slot in range(SLOTS)])
        for slot in range(SLOTS):
            for at in range(COL_SHARDS):
                pltpu.make_async_remote_copy(
                    src_ref=images.at[turn, slot], dst_ref=image_near.at[turn, slot, at],
                    send_sem=image_send.at[turn, slot, at], recv_sem=image_recv.at[turn, slot, at],
                    device_id=sibling, device_id_type=MESH_ID,
                ).wait_recv()
        near = rows_of([image_near[turn, slot, 0] + image_near[turn, slot, 1] for slot in range(SLOTS)])
        directions = own - near

        stats[turn, shard] = gram(directions)
        stat_copies = [
            send(
                stats.at[turn, shard], stats.at[turn, shard],
                stat_send.at[turn, apart], stat_recv.at[turn, apart], peer,
            )
            for apart, peer in enumerate(shard_peers)
        ]
        direction_halves = stacked_halves(directions)
        projection = product(direction_halves, x[...], NN)
        projection = projection[:EDGE_ROWS] + projection[EDGE_ROWS:]
        if turn > 0:
            overlap = product(direction_halves, stacked_halves(lefts[0]), NT)
            overlap = overlap[:EDGE_ROWS] + overlap[EDGE_ROWS:]
            overlap = overlap[:, :EDGE_ROWS] + overlap[:, EDGE_ROWS:]
            for g in range(EDGE_ROWS):
                projection = projection + overlap[:, g : g + 1] * rights[0][g : g + 1, :]
        for part in range(ROW_SHARDS):
            parts[turn, part] = projection[:, part * quarter : (part + 1) * quarter]
        part_copies = []
        for apart, peer in enumerate(shard_peers):
            part_copies.append(
                send(
                    parts.at[turn, (shard + apart + 1) % ROW_SHARDS], parts_in.at[turn, apart],
                    part_send.at[turn, apart], part_recv.at[turn, apart], peer,
                )
            )
        for copy in part_copies:
            copy.wait_recv()
        total = parts[turn, shard]
        for apart in range(ROW_SHARDS - 1):
            total = total + parts_in[turn, apart]
        for slot in range(SLOTS):
            sums[turn, slot] = total[RANK * slot : RANK * (slot + 1), :]
        sum_copies = []
        for slot, node in enumerate(neighbours):
            sum_copies.append(
                send(
                    sums.at[turn, slot], sums_in.at[turn, slot ^ 1],
                    sum_send.at[turn, slot], sum_recv.at[turn, slot ^ 1],
                    device(node, shard, core),
                )
            )
        for copy in stat_copies:
            copy.wait_recv()
        statistics = (stats[turn, 0] + stats[turn, 1]) + (stats[turn, 2] + stats[turn, 3])
        scale, share = normalizers(statistics)
        lefts.append(normalized(directions, scale, share))
        for copy in sum_copies:
            copy.wait_recv()
        total = total + rows_of([sums_in[turn, slot] for slot in range(SLOTS)])
        shares[turn, shard] = normalized(total, scale, share)
        share_copies = [
            send(
                shares.at[turn, shard], shares.at[turn, shard],
                share_send.at[turn, apart], share_recv.at[turn, apart], peer,
            )
            for apart, peer in enumerate(shard_peers)
        ]
        if turn == ROUNDS - 1:
            left_out[...] = jnp.concatenate(lefts, axis=0)
        for copy in share_copies:
            copy.wait_recv()
        factors = jnp.concatenate([shares[turn, part] for part in range(ROW_SHARDS)], axis=1)
        rights.append(weight * factors)
    right_out[...] = jnp.concatenate(rights, axis=0)
    for copy in sent:
        copy.wait_send()


def outer(left_ref, right_ref, out_hbm, block, sem):
    left_high, left_low = halves(left_ref[...])
    left = jnp.concatenate([left_high, left_high, left_low], axis=0)
    chunk = block.shape[2]
    copies = []
    for step in range(block.shape[0]):
        at = pl.ds(step * chunk, chunk)
        right_high, right_low = halves(right_ref[:, at])
        right = jnp.concatenate([right_high, right_low, right_high], axis=0)
        block[step] = product(left, right, TN)
        copy = pltpu.make_async_copy(block.at[step], out_hbm.at[:, at], sem.at[step])
        copy.start()
        copies.append(copy)
    for copy in copies:
        copy.wait()


def per_device(replicas, factor_seeds, edge_counts):
    rows, width = replicas.shape
    quarter = width // ROW_SHARDS
    both = ROUNDS * EDGE_ROWS
    peers = ROW_SHARDS - 1
    f32 = jnp.float32
    dma = pltpu.SemaphoreType.DMA
    left, right = pl.pallas_call(
        consensus,
        out_shape=[
            jax.ShapeDtypeStruct((both, rows), f32),
            jax.ShapeDtypeStruct((both, width), f32),
        ],
        in_specs=[
            pl.BlockSpec(memory_space=pl.ANY),
            pl.BlockSpec(memory_space=pltpu.SMEM),
            pl.BlockSpec(memory_space=pltpu.SMEM),
        ],
        out_specs=[pl.BlockSpec(memory_space=pltpu.VMEM)] * 2,
        scratch_shapes=[
            pltpu.VMEM((rows, width), replicas.dtype),
            pltpu.VMEM((ROUNDS, SLOTS, RANK, rows), f32),
            pltpu.VMEM((ROUNDS, SLOTS, RANK, rows), f32),
            pltpu.VMEM((ROUNDS, SLOTS, COL_SHARDS, RANK, rows), f32),
            pltpu.VMEM((ROUNDS, ROW_SHARDS, EDGE_ROWS, 128), f32),
            pltpu.VMEM((ROUNDS, ROW_SHARDS, EDGE_ROWS, quarter), f32),
            pltpu.VMEM((ROUNDS, peers, EDGE_ROWS, quarter), f32),
            pltpu.VMEM((ROUNDS, SLOTS, RANK, quarter), f32),
            pltpu.VMEM((ROUNDS, SLOTS, RANK, quarter), f32),
            pltpu.VMEM((ROUNDS, ROW_SHARDS, EDGE_ROWS, quarter), f32),
            dma,
            dma((ROUNDS, SLOTS + 1, COL_SHARDS)),
            dma((ROUNDS, SLOTS + 1, COL_SHARDS)),
            dma((ROUNDS, peers)),
            dma((ROUNDS, peers)),
            dma((ROUNDS, peers)),
            dma((ROUNDS, peers)),
            dma((ROUNDS, SLOTS)),
            dma((ROUNDS, SLOTS)),
            dma((ROUNDS, peers)),
            dma((ROUNDS, peers)),
        ],
        compiler_params=pltpu.CompilerParams(collective_id=0, has_side_effects=True),
        name="consensus",
    )(replicas, factor_seeds, edge_counts)
    chunks = 5
    return pl.pallas_call(
        outer,
        out_shape=jax.ShapeDtypeStruct((rows, width), f32),
        in_specs=[pl.BlockSpec(memory_space=pltpu.VMEM)] * 2,
        out_specs=pl.BlockSpec(memory_space=pl.ANY),
        scratch_shapes=[pltpu.VMEM((chunks, rows, width // chunks), f32), dma((chunks,))],
        name="outer",
    )(left, right)


def solution(mesh):
    return jax.shard_map(
        per_device,
        mesh=mesh,
        in_specs=(P("row", "col"), P(), P()),
        out_specs=P("row", "col"),
        check_vma=False,
    )
```

```python
import functools

import jax
import jax.numpy as jnp
from jax import lax
from jax.experimental import pallas as pl
from jax.experimental.pallas import tpu as pltpu
from jax.sharding import PartitionSpec as P

ROUNDS = 2
ROW_SHARDS = 4
COL_SHARDS = 2
SLOTS = 4
RANK = 2
EDGE_ROWS = SLOTS * RANK
PRIME = 8191
EPSILON = 1e-06
VMEM_BYTES = 12 << 20
PART_ORDER = (2, 1, 3, 0)
MESH_ID = pl.DeviceIdType.MESH
NT = (((1,), (1,)), ((), ()))
NN = (((1,), (0,)), ((), ()))
TN = (((0,), (0,)), ((), ()))


def product(left, right, dims):
    return lax.dot_general(left, right, dims, preferred_element_type=jnp.float32)


def halves(values):
    high = values.astype(jnp.bfloat16)
    return high, (values - high.astype(jnp.float32)).astype(jnp.bfloat16)


def stacked_halves(values):
    return jnp.concatenate(halves(values), axis=0)


def folded(values):
    return (values & PRIME) + (values >> 13)


def start_factors(seed_column, first_column, width):
    column = first_column + lax.broadcasted_iota(jnp.int32, (EDGE_ROWS, width), 1)
    square = folded(column * column)
    residue = folded(folded(square * (seed_column + 1) + column * 17))
    residue = jnp.where(residue >= PRIME, residue - PRIME, residue)
    return residue.astype(jnp.float32) * (2.0 / 8191.0) - 1.0


def column_of(scalars):
    row = lax.broadcasted_iota(jnp.int32, (EDGE_ROWS, 1), 0)
    values = jnp.full((EDGE_ROWS, 1), scalars[0])
    for index in range(1, EDGE_ROWS):
        values = jnp.where(row == index, scalars[index], values)
    return values


def partner_rows(values):
    row = lax.broadcasted_iota(jnp.int32, values.shape, 0)
    down = pltpu.roll(values, 1, 0)
    up = pltpu.roll(values, EDGE_ROWS - 1, 0)
    return jnp.where(row % 2 == 0, up, down)


def gram(directions):
    norm = jnp.sum(directions * directions, axis=1, keepdims=True)
    cross = jnp.sum(directions * partner_rows(directions), axis=1, keepdims=True)
    lane = lax.broadcasted_iota(jnp.int32, (EDGE_ROWS, 128), 1)
    return jnp.where(lane == 0, norm, jnp.where(lane == 1, cross, 0.0))


def normalizers(statistics):
    row = lax.broadcasted_iota(jnp.int32, (EDGE_ROWS, 128), 0)
    norm = jnp.broadcast_to(statistics[:, 0:1], (EDGE_ROWS, 128))
    cross = jnp.broadcast_to(statistics[:, 1:2], (EDGE_ROWS, 128))
    other = partner_rows(norm)
    first = row % 2 == 0
    lead = jnp.where(first, norm, other)
    rest = jnp.where(first, other, norm)
    share = jnp.where(cross == lead + EPSILON, 1.0, cross / (lead + EPSILON))
    left_over = (rest - share * cross) - share * (cross - share * lead)
    left_over = jnp.maximum(left_over, 0.0)
    scale = 1.0 / jnp.sqrt(jnp.where(first, lead, left_over) + EPSILON)
    share = jnp.where(first, 0.0, share)
    return scale[:, 0:1], share[:, 0:1]


def normalized(values, scale, share):
    return (values - share * partner_rows(values)) * scale


def rows_of(slabs):
    return jnp.concatenate([slabs[slot] for slot in range(SLOTS)], axis=0)


def consensus(
    x_hbm, seeds_hbm, counts_hbm, left_out, right_out, x, seeds, counts, images, image_pair, image_near,
    stats, parts, parts_in, sums, sums_in, shares, load_sem, image_send, image_recv,
    stat_send, stat_recv, part_send, part_recv, sum_send, sum_recv, share_send, share_recv,
):
    quarter = x.shape[2]
    width = ROW_SHARDS * quarter
    graph_rows, graph_cols = seeds.shape[0], seeds.shape[3]
    row, col = lax.axis_index("row"), lax.axis_index("col")
    node_row, shard = row // ROW_SHARDS, row % ROW_SHARDS
    node_col, core = col // COL_SHARDS, col % COL_SHARDS
    below = (node_row + 1) % graph_rows
    above = (node_row + graph_rows - 1) % graph_rows
    right = (node_col + 1) % graph_cols
    left = (node_col + graph_cols - 1) % graph_cols
    neighbours = [(below, node_col), (above, node_col), (node_row, right), (node_row, left)]

    def device(node, at_shard, at_core):
        return (node[0] * ROW_SHARDS + at_shard, node[1] * COL_SHARDS + at_core)

    sibling = device((node_row, node_col), shard, 1 - core)
    shard_peers = [
        device((node_row, node_col), (shard + apart) % ROW_SHARDS, core)
        for apart in range(1, ROW_SHARDS)
    ]

    barrier = pltpu.get_barrier_semaphore()
    partners = [device(node, shard, at) for node in neighbours for at in range(COL_SHARDS)]
    partners += [sibling] + shard_peers
    for partner in partners:
        pl.semaphore_signal(barrier, inc=1, device_id=partner, device_id_type=MESH_ID)
    sources = [seeds_hbm, counts_hbm] + [x_hbm.at[:, pl.ds(part * quarter, quarter)] for part in range(ROW_SHARDS)]
    targets = [seeds, counts] + [x.at[part] for part in range(ROW_SHARDS)]
    loads = [
        pltpu.make_async_copy(source, target, load_sem.at[index])
        for index, (source, target) in enumerate(zip(sources, targets))
    ]
    for load in loads:
        load.start()

    loads[0].wait()
    loads[1].wait()
    owners = [(node_row, node_col, 0), (above, node_col, 0), (node_row, node_col, 1), (node_row, left, 1)]
    seed_column = column_of([seeds[r, a, k, c] for r, c, a in owners for k in range(RANK)])
    weight = column_of([counts[r, a, c] for r, c, a in owners for _ in range(RANK)])
    weight = weight.astype(jnp.float32) * (-1.0 / 16.0)
    factors = start_factors(seed_column, core * width, width)

    sent = []

    def send(source, target, send_sem, recv_sem, to):
        copy = pltpu.make_async_remote_copy(
            src_ref=source, dst_ref=target, send_sem=send_sem, recv_sem=recv_sem,
            device_id=to, device_id_type=MESH_ID,
        )
        copy.start()
        sent.append(copy)
        return copy

    lefts = []
    share_copies = None
    for turn in range(ROUNDS):
        image = None
        overlap = None
        for step in range(ROW_SHARDS):
            if turn == 0:
                part = step
                loads[2 + part].wait()
                factor = factors[:, part * quarter : (part + 1) * quarter]
            else:
                part = (shard + ROW_SHARDS - step) % ROW_SHARDS
                if step > 0:
                    share_copies[step - 1].wait_recv()
                factor = shares[turn - 1, part]
            factor_halves = stacked_halves(factor)
            term = product(factor_halves, x[part], NT)
            image = term if image is None else image + term
            if turn > 0:
                term = product(factor_halves, factor_halves, NT)
                overlap = term if overlap is None else overlap + term
        image = image[:EDGE_ROWS] + image[EDGE_ROWS:]
        if turn > 0:
            overlap = overlap[:EDGE_ROWS] + overlap[EDGE_ROWS:]
            overlap = overlap[:, :EDGE_ROWS] + overlap[:, EDGE_ROWS:]
            weighted = weight * lefts[0]
            for g in range(EDGE_ROWS):
                image = image + overlap[:, g : g + 1] * weighted[g : g + 1, :]
        for slot in range(SLOTS):
            images[turn, slot] = image[RANK * slot : RANK * (slot + 1), :]
        if turn == 0:
            pl.semaphore_wait(barrier, len(partners))
        arrivals = []
        for slot, node in enumerate(neighbours):
            for at in range(COL_SHARDS):
                arrivals.append(
                    send(
                        images.at[turn, slot], image_near.at[turn, slot ^ 1, core],
                        image_send.at[turn, slot, at], image_recv.at[turn, slot ^ 1, core],
                        device(node, shard, at),
                    )
                )
        pair = send(images.at[turn], image_pair.at[turn], image_send.at[turn, SLOTS, 0], image_recv.at[turn, SLOTS, 0], sibling)
        pair.wait_recv()
        own = image + rows_of([image_pair[turn, slot] for slot in range(SLOTS)])
        for slot in range(SLOTS):
            for at in range(COL_SHARDS):
                pltpu.make_async_remote_copy(
                    src_ref=images.at[turn, slot], dst_ref=image_near.at[turn, slot, at],
                    send_sem=image_send.at[turn, slot, at], recv_sem=image_recv.at[turn, slot, at],
                    device_id=sibling, device_id_type=MESH_ID,
                ).wait_recv()
        near = rows_of([image_near[turn, slot, 0] + image_near[turn, slot, 1] for slot in range(SLOTS)])
        directions = own - near

        direction_halves = stacked_halves(directions)
        if turn > 0:
            overlap = product(direction_halves, stacked_halves(lefts[0]), NT)
            overlap = overlap[:EDGE_ROWS] + overlap[EDGE_ROWS:]
            overlap = overlap[:, :EDGE_ROWS] + overlap[:, EDGE_ROWS:]
        part_copies = []
        for apart in PART_ORDER:
            part = (shard + apart) % ROW_SHARDS
            projection = product(direction_halves, x[part], NN)
            projection = projection[:EDGE_ROWS] + projection[EDGE_ROWS:]
            if turn > 0:
                weighted = weight * shares[0, part]
                for g in range(EDGE_ROWS):
                    projection = projection + overlap[:, g : g + 1] * weighted[g : g + 1, :]
            parts[turn, part] = projection
            if apart > 0:
                part_copies.append(
                    send(
                        parts.at[turn, part], parts_in.at[turn, apart - 1],
                        part_send.at[turn, apart - 1], part_recv.at[turn, apart - 1], shard_peers[apart - 1],
                    )
                )
        stats[turn, shard] = gram(directions)
        stat_copies = [
            send(
                stats.at[turn, shard], stats.at[turn, shard],
                stat_send.at[turn, apart], stat_recv.at[turn, apart], peer,
            )
            for apart, peer in enumerate(shard_peers)
        ]
        for copy in part_copies:
            copy.wait_recv()
        total = parts[turn, shard]
        for apart in range(ROW_SHARDS - 1):
            total = total + parts_in[turn, apart]
        for slot in range(SLOTS):
            sums[turn, slot] = total[RANK * slot : RANK * (slot + 1), :]
        sum_copies = []
        for slot, node in enumerate(neighbours):
            sum_copies.append(
                send(
                    sums.at[turn, slot], sums_in.at[turn, slot ^ 1],
                    sum_send.at[turn, slot], sum_recv.at[turn, slot ^ 1],
                    device(node, shard, core),
                )
            )
        for copy in stat_copies:
            copy.wait_recv()
        statistics = (stats[turn, 0] + stats[turn, 1]) + (stats[turn, 2] + stats[turn, 3])
        scale, share = normalizers(statistics)
        lefts.append(normalized(directions, scale, share))
        for copy in sum_copies:
            copy.wait_recv()
        total = total + rows_of([sums_in[turn, slot] for slot in range(SLOTS)])
        shares[turn, shard] = normalized(total, scale, share)
        share_copies = [
            send(
                shares.at[turn, shard], shares.at[turn, shard],
                share_send.at[turn, apart], share_recv.at[turn, apart], peer,
            )
            for apart, peer in enumerate(shard_peers)
        ]
    left_out[...] = jnp.concatenate(lefts, axis=0)
    for copy in share_copies:
        copy.wait_recv()
    for turn in range(ROUNDS):
        for part in range(ROW_SHARDS):
            at = slice(part * quarter, (part + 1) * quarter)
            right_out[turn * EDGE_ROWS : (turn + 1) * EDGE_ROWS, at] = weight * shares[turn, part]
    for copy in sent:
        copy.wait_send()


def outer(left_ref, right_ref, out_hbm, block, sem):
    left_high, left_low = halves(left_ref[...])
    left = jnp.concatenate([left_high, left_high, left_low], axis=0)
    chunk = block.shape[2]
    copies = []
    for step in range(block.shape[0]):
        at = pl.ds(step * chunk, chunk)
        right_high, right_low = halves(right_ref[:, at])
        right = jnp.concatenate([right_high, right_low, right_high], axis=0)
        block[step] = product(left, right, TN)
        copy = pltpu.make_async_copy(block.at[step], out_hbm.at[:, at], sem.at[step])
        copy.start()
        copies.append(copy)
    for copy in copies:
        copy.wait()


def per_device(replicas, factor_seeds, edge_counts):
    rows, width = replicas.shape
    quarter = width // ROW_SHARDS
    both = ROUNDS * EDGE_ROWS
    peers = ROW_SHARDS - 1
    f32 = jnp.float32
    dma = pltpu.SemaphoreType.DMA
    factor_seeds = factor_seeds.transpose(0, 2, 3, 1)
    edge_counts = edge_counts.transpose(0, 2, 1)
    left, right = pl.pallas_call(
        consensus,
        out_shape=[
            jax.ShapeDtypeStruct((both, rows), f32),
            jax.ShapeDtypeStruct((both, width), f32),
        ],
        in_specs=[
            pl.BlockSpec(memory_space=pltpu.HBM),
            pl.BlockSpec(memory_space=pltpu.HBM),
            pl.BlockSpec(memory_space=pltpu.HBM),
        ],
        out_specs=[pl.BlockSpec(memory_space=pltpu.VMEM)] * 2,
        scratch_shapes=[
            pltpu.VMEM((ROW_SHARDS, rows, quarter), replicas.dtype),
            pltpu.SMEM(factor_seeds.shape, jnp.int32),
            pltpu.SMEM(edge_counts.shape, jnp.int32),
            pltpu.VMEM((ROUNDS, SLOTS, RANK, rows), f32),
            pltpu.VMEM((ROUNDS, SLOTS, RANK, rows), f32),
            pltpu.VMEM((ROUNDS, SLOTS, COL_SHARDS, RANK, rows), f32),
            pltpu.VMEM((ROUNDS, ROW_SHARDS, EDGE_ROWS, 128), f32),
            pltpu.VMEM((ROUNDS, ROW_SHARDS, EDGE_ROWS, quarter), f32),
            pltpu.VMEM((ROUNDS, peers, EDGE_ROWS, quarter), f32),
            pltpu.VMEM((ROUNDS, SLOTS, RANK, quarter), f32),
            pltpu.VMEM((ROUNDS, SLOTS, RANK, quarter), f32),
            pltpu.VMEM((ROUNDS, ROW_SHARDS, EDGE_ROWS, quarter), f32),
            dma((2 + ROW_SHARDS,)),
            dma((ROUNDS, SLOTS + 1, COL_SHARDS)),
            dma((ROUNDS, SLOTS + 1, COL_SHARDS)),
            dma((ROUNDS, peers)),
            dma((ROUNDS, peers)),
            dma((ROUNDS, peers)),
            dma((ROUNDS, peers)),
            dma((ROUNDS, SLOTS)),
            dma((ROUNDS, SLOTS)),
            dma((ROUNDS, peers)),
            dma((ROUNDS, peers)),
        ],
        compiler_params=pltpu.CompilerParams(collective_id=0, has_side_effects=True, vmem_limit_bytes=VMEM_BYTES),
        name="consensus",
    )(*(pltpu.with_memory_space_constraint(v, pltpu.HBM) for v in (replicas, factor_seeds, edge_counts)))
    chunks = 5
    return pl.pallas_call(
        outer,
        out_shape=jax.ShapeDtypeStruct((rows, width), f32),
        in_specs=[pl.BlockSpec(memory_space=pltpu.VMEM)] * 2,
        out_specs=pl.BlockSpec(memory_space=pl.ANY),
        scratch_shapes=[pltpu.VMEM((chunks, rows, width // chunks), f32), dma((chunks,))],
        compiler_params=pltpu.CompilerParams(vmem_limit_bytes=VMEM_BYTES),
        name="outer",
    )(left, right)


def solution(mesh):
    return jax.shard_map(
        per_device,
        mesh=mesh,
        in_specs=(P("row", "col"), P(), P()),
        out_specs=P("row", "col"),
        check_vma=False,
    )
```
